256 devices in a mesh: grp: 8 (over y, core), dev: 32 (over x, z).
Axes of the slice: x: 4, y: 4, z: 8, core: 2. Of those that a mesh axis runs over, the one named last changes fastest.
Arguments:
- densities: bfloat16 [256, 200, 200], P(('grp', 'dev')), may hold values from -0.4375 to 0.4375
- core_hamiltonian: bfloat16 [256, 200, 200], P(('grp', 'dev')), may hold values from -0.21875 to 0.21875
- embedding: bfloat16 [256, 200, 200], P(('grp', 'dev')), may hold values from -0.21875 to 0.21875
- fit_factors: bfloat16 [768, 200, 200], P('dev'), may hold values from -0.059814453 to 0.059814453
- orthogonalizers: bfloat16 [256, 200, 200], P(('grp', 'dev'))
- pairs: int32 [3072, 2], replicated, may hold values from 0 to 255, as said below
- assignment: int32 [3072], replicated, may hold values from 0 to 31, as said below
- owner_map: int32 [256], replicated, may hold values from 0 to 255, as said below
Outputs:
- slot_energies: float32 [6144], P(('grp', 'dev'))
- total: float32 [], replicated
The draws below stay inside these ranges and needn't reach their ends.
Inputs may be any that keep to these rules, and one draw needn't show every extreme that they name: `pairs`: dimer k belongs to group g = k // 384; its first fragment lies in block g, the fragments g * 32 to (g + 1) * 32 - 1, and its second fragment, different from the first, lies in block g or block g + 1 (only block g for the last group). `assignment`: no device receives more than 24 dimers of its group, and in every group some device receives exactly 24. `owner_map`: A permutation of the fragments that maps each block of 32 fragments onto the rows of the same block.
All inputs are finite; a program needn't handle non-finite values.
Results may differ from the reference program's by a relative error of at most 0.0003.
Values may be sent and summed in bfloat16 or wider, within the bound.
No kernel may reach another device: no remote copies, remote signals or barrier semaphores. Data moves between devices by JAX's collectives and lax.ppermute only.
A program may use at most 128 MiB of HBM per device.

```python
import jax
import jax.numpy as jnp
from jax import lax

NB = 200
SLOTS = 24
BLOCK = 32
FRAGS = 256
NAUX = 768
DIM_GRP = 384
NDIMERS = 3072
SLOT_ALL = 6144


def draw_pairs(key, part):
    base = jax.random.fold_in(key, 11)
    key_first, key_next, key_same, key_far = jax.random.split(base, 4)
    group_count = FRAGS // BLOCK
    group_ids = jnp.arange(NDIMERS, dtype=jnp.int32) // DIM_GRP
    first_local = jax.random.randint(key_first, (NDIMERS,), 0, BLOCK, dtype=jnp.int32)
    go_next = (jax.random.randint(key_next, (NDIMERS,), 0, 2, dtype=jnp.int32) == 1) & (group_ids < group_count - 1)
    offset = jax.random.randint(key_same, (NDIMERS,), 0, BLOCK - 1, dtype=jnp.int32)
    same_local = (first_local + 1 + offset) % BLOCK
    next_local = jax.random.randint(key_far, (NDIMERS,), 0, BLOCK, dtype=jnp.int32)
    second = jnp.where(go_next, (group_ids + 1) * BLOCK + next_local, group_ids * BLOCK + same_local)
    first = group_ids * BLOCK + first_local
    return jnp.stack([first, second], axis=1).astype(jnp.int32)


def draw_assignment(key, part):
    group_count = FRAGS // BLOCK
    token_count = BLOCK * SLOTS
    tokens = jnp.arange(token_count, dtype=jnp.int32) // SLOTS
    positions = jnp.arange(token_count, dtype=jnp.int32)

    def one_group(group_key):
        key_busy, key_score, key_perm = jax.random.split(group_key, 3)
        busiest = jax.random.randint(key_busy, (), 0, BLOCK, dtype=jnp.int32)
        scores = jax.random.randint(key_score, (token_count,), 0, 2 ** 20, dtype=jnp.int32)
        ranking = jnp.where(tokens == busiest, positions, token_count + scores * token_count + positions)
        order = jnp.argsort(ranking, stable=True)
        chosen = tokens[order[:DIM_GRP]]
        shuffle = jax.random.permutation(key_perm, DIM_GRP)
        return chosen[shuffle]
    group_keys = jax.random.split(jax.random.fold_in(key, 23), group_count)
    return jax.vmap(one_group)(group_keys).reshape(-1).astype(jnp.int32)


def draw_owner_map(key, part):
    group_count = FRAGS // BLOCK
    group_keys = jax.random.split(jax.random.fold_in(key, 37), group_count)
    perms = jax.vmap(lambda group_key: jax.random.permutation(group_key, BLOCK))(group_keys)
    shifted = perms + jnp.arange(group_count, dtype=jnp.int32)[:, None] * BLOCK
    return shifted.reshape(-1).astype(jnp.int32)


def draw_orthogonalizers(key, part):
    noise_key = jax.random.fold_in(key, 41)
    shape = (FRAGS, NB, NB)
    noise = jax.random.truncated_normal(noise_key, -3.0, 3.0, shape, jnp.float32)
    identity = jnp.eye(NB, dtype=jnp.float32)[None, :, :]
    return (identity + 0.4 * noise / jnp.sqrt(jnp.float32(NB))).astype(jnp.bfloat16)


def shard_levels(own_key, dims, cuts, low, largest):
    def one(position, blocks):
        heights = jax.random.uniform(jax.random.fold_in(jax.random.fold_in(own_key, 6), position), (blocks,), jnp.float32, low / len(cuts), largest / len(cuts))
        return jnp.repeat(jnp.exp(heights), dims[position] // blocks).reshape((-1,) + (1,) * (len(dims) - position - 1))

    loudness = one(*cuts[0])
    for cut in cuts[1:]:
        loudness = loudness * one(*cut)
    return loudness


def gaussian(rng, extent, deviation, limit, cuts=(), kind=jnp.bfloat16):
    entries = deviation * jax.random.normal(rng, extent, jnp.float32)
    if cuts:
        entries = entries * shard_levels(rng, extent, cuts, -0.22, 0.18)
    return jnp.clip(entries, -limit, limit).astype(kind)


def setup_inputs(seed: int = 0) -> dict:
    streams_of = jax.random.split(jax.random.key(seed), 9)
    densities = gaussian(streams_of[0], (FRAGS, NB, NB), NB ** -0.5, 0.4375, ((0, 256),))
    core_hamiltonian = gaussian(streams_of[1], (FRAGS, NB, NB), (4 * NB) ** -0.5, 0.21875, ((0, 256),))
    embedding = gaussian(streams_of[2], (FRAGS, NB, NB), (4 * NB) ** -0.5, 0.21875, ((0, 256),))
    fit_factors = gaussian(streams_of[3], (NAUX, NB, NB), 0.01, 0.059814453, ((0, 32),))
    orthogonalizers = draw_orthogonalizers(jax.random.fold_in(streams_of[8], 71), 0)
    pairs = draw_pairs(jax.random.fold_in(streams_of[8], 71), 0)
    assignment = draw_assignment(jax.random.fold_in(streams_of[8], 71), 0)
    owner_map = draw_owner_map(jax.random.fold_in(streams_of[8], 71), 0)
    return dict(densities=densities, core_hamiltonian=core_hamiltonian, embedding=embedding, fit_factors=fit_factors, orthogonalizers=orthogonalizers, pairs=pairs, assignment=assignment, owner_map=owner_map)


HALF_WIDTH = 4.0


def product(left, right):
    return jnp.dot(left, right, preferred_element_type=jnp.float32)


def dimer_energy(fock_i, fock_j, dens_i, dens_j, ortho_i, ortho_j):
    coupling = (0.5 * (product(fock_i, dens_j) + product(dens_i, fock_j))).astype(jnp.bfloat16)
    upper_left = product(fock_i, ortho_i).astype(jnp.bfloat16)
    upper_right = product(coupling, ortho_j).astype(jnp.bfloat16)
    lower_left = product(coupling.T, ortho_i).astype(jnp.bfloat16)
    lower_right = product(fock_j, ortho_j).astype(jnp.bfloat16)
    top_rows = jnp.concatenate([product(ortho_i.T, upper_left), product(ortho_i.T, upper_right)], axis=1)
    bottom_rows = jnp.concatenate([product(ortho_j.T, lower_left), product(ortho_j.T, lower_right)], axis=1)
    ortho_fock = jnp.concatenate([top_rows, bottom_rows], axis=0)
    size_two = ortho_fock.shape[0]
    half_basis = fock_i.shape[0]
    start = (0.5 * jnp.eye(size_two, dtype=jnp.float32) - ortho_fock / (2.0 * HALF_WIDTH)).astype(jnp.bfloat16)
    square = product(start, start).astype(jnp.bfloat16)
    cube = product(square, start)
    purified = (3.0 * square.astype(jnp.float32) - 2.0 * cube).astype(jnp.bfloat16)
    left_part = jnp.concatenate([product(ortho_i, purified[:half_basis]), product(ortho_j, purified[half_basis:])], axis=0).astype(jnp.bfloat16)
    new_density = jnp.concatenate([product(left_part[:, :half_basis], ortho_i.T), product(left_part[:, half_basis:], ortho_j.T)], axis=1)
    fock_top = jnp.concatenate([fock_i, coupling], axis=1)
    fock_bottom = jnp.concatenate([coupling.T, fock_j], axis=1)
    dimer_fock = jnp.concatenate([fock_top, fock_bottom], axis=0).astype(jnp.float32)
    monomer_i = jnp.sum(dens_i.astype(jnp.float32) * fock_i.astype(jnp.float32))
    monomer_j = jnp.sum(dens_j.astype(jnp.float32) * fock_j.astype(jnp.float32))
    return jnp.sum(new_density * dimer_fock) - monomer_i - monomer_j


def reference(densities, core_hamiltonian, embedding, fit_factors, orthogonalizers, pairs, assignment, owner_map):
    flat_dens = densities.reshape(FRAGS, NB * NB)
    flat_fit = fit_factors.reshape(NAUX, NB * NB)
    coeffs = lax.dot_general(flat_dens, flat_fit, (((1,), (1,)), ((), ())), preferred_element_type=jnp.float32).astype(jnp.bfloat16)
    coulomb = jnp.dot(coeffs, flat_fit, preferred_element_type=jnp.float32).reshape(FRAGS, NB, NB)
    fock_rows = (core_hamiltonian.astype(jnp.float32) + embedding.astype(jnp.float32) + coulomb).astype(jnp.bfloat16)
    row_pairs = owner_map[pairs].astype(jnp.int32)

    def one_dimer(row_pair):
        first_row = row_pair[0]
        second_row = row_pair[1]
        return dimer_energy(fock_rows[first_row], fock_rows[second_row], densities[first_row], densities[second_row], orthogonalizers[first_row], orthogonalizers[second_row])

    energies = lax.map(one_dimer, row_pairs)
    groups = NDIMERS // DIM_GRP
    group_assign = assignment.reshape(groups, DIM_GRP)
    onehot = (group_assign[:, :, None] == jnp.arange(BLOCK, dtype=jnp.int32)[None, None, :]).astype(jnp.int32)
    earlier = jnp.cumsum(onehot, axis=1) - onehot
    rank = jnp.sum(earlier * onehot, axis=2).astype(jnp.int32)
    group_ids = (jnp.arange(NDIMERS, dtype=jnp.int32) // DIM_GRP).astype(jnp.int32)
    slot_index = ((group_ids * BLOCK + assignment) * SLOTS + rank.reshape(-1)).astype(jnp.int32)
    slot_energies = jnp.zeros((SLOT_ALL,), jnp.float32).at[slot_index].set(energies)
    total = jnp.sum(energies)
    return (slot_energies, total)
```

```python
import functools

import jax
import jax.numpy as jnp
from jax import lax
from jax.experimental import pallas as pl
from jax.experimental.pallas import tpu as pltpu
from jax.sharding import Mesh
from jax.sharding import PartitionSpec as P

SLOTS = 24
LANES = 128
DEV = ("dev_0", "dev_1")
GRP_DEV = ("grp", "dev_0", "dev_1")
HALF_WIDTH = 4.0


def moved(block, axis, distance):
    count = lax.axis_size(axis)
    return lax.ppermute(block, axis, [(i, (i + distance) % count) for i in range(count)])


def from_behind(block, axis, distance):
    devices = range(lax.axis_size(axis))
    route = [(i - distance, i) for i in devices if i - distance in devices]
    return lax.ppermute(block, axis, route)


def along_ring(block, axis):
    half = lax.axis_size(axis) // 2
    behind, ahead = [block], [block]
    for _ in range(half - 1):
        behind.append(moved(behind[-1], axis, 1))
        ahead.append(moved(ahead[-1], axis, -1))
    cut = block.shape[0] // 2
    far = jnp.concatenate([moved(behind[-1][:cut], axis, 1), moved(ahead[-1][cut:], axis, -1)])
    return behind + [far] + ahead[:0:-1]


def along_line(block, axis):
    return [block] + [moved(block, axis, k) for k in range(1, lax.axis_size(axis))]


def summed_behind(terms, axis):
    arrived = [terms[0]] + [moved(terms[k], axis, -k) for k in range(1, lax.axis_size(axis))]
    return functools.reduce(jnp.add, [a.astype(jnp.float32) for a in arrived])


def summed_columns(terms, axis):
    cut = terms[0].shape[1] // 16 * 8 + 8
    low, high = [t[:, :cut] for t in terms], [t[:, cut:] for t in terms]
    passing_down = moved(low[2], axis, -1)
    passing_up = moved(high[2], axis, 1)
    high_down = moved(high[1], axis, -1)
    low_up = moved(low[3], axis, 1)
    low_down = moved(added(low[1], passing_down), axis, -1)
    high_up = moved(added(high[3], passing_up), axis, 1)
    return jnp.concatenate(
        [added(low[0], low_up, low_down), added(high[0], high_up, high_down)], axis=1
    )


def added(*arrays):
    return functools.reduce(jnp.add, [a.astype(jnp.float32) for a in arrays]).astype(jnp.bfloat16)


def sent_to_all(array, axis):
    copies = jnp.broadcast_to(array, (lax.axis_size(axis), *array.shape))
    return lax.all_to_all(copies, axis, split_axis=0, concat_axis=0, tiled=True)


def product(left, right):
    return jnp.dot(left, right, preferred_element_type=jnp.float32)


def turned(left, right):
    return lax.dot_general(
        left, right, (((0,), (0,)), ((), ())), preferred_element_type=jnp.float32
    )


def stage(function, *lists):
    return [function(*items) for items in zip(*lists)]


def dimer_terms(operands):
    size = operands[0][0].shape[0]
    low = jnp.bfloat16
    rows = lax.broadcasted_iota(jnp.int32, (size, size), 0)
    columns = lax.broadcasted_iota(jnp.int32, (size, size), 1)
    middle = jnp.where(rows == columns, 0.5, 0.0).astype(jnp.float32)
    scale = 1.0 / (2.0 * HALF_WIDTH)

    def ortho_blocks(item):
        fock_i, dens_i, ortho_i, fock_j, dens_j, ortho_j = item
        half_ii = product(fock_i, ortho_i).astype(low)
        half_jj = product(fock_j, ortho_j).astype(low)
        coupling = (0.5 * (product(fock_i, dens_j) + product(dens_i, fock_j))).astype(low)
        half_ij = product(coupling, ortho_j).astype(low)
        return turned(ortho_i, half_ii), turned(ortho_i, half_ij), turned(ortho_j, half_jj)

    def starts(blocks):
        o_ii, o_ij, o_jj = blocks
        s_ij = -o_ij * scale
        return (
            (middle - o_ii * scale).astype(low),
            s_ij.astype(low),
            s_ij.T.astype(low),
            (middle - o_jj * scale).astype(low),
        )

    def times(a, b):
        return (
            product(a[0], b[0]) + product(a[1], b[2]),
            product(a[0], b[1]) + product(a[1], b[3]),
            product(a[2], b[0]) + product(a[3], b[2]),
            product(a[2], b[1]) + product(a[3], b[3]),
        )

    def purified(q, c):
        return (3.0 * q.astype(jnp.float32) - 2.0 * c).astype(low).astype(jnp.float32)

    def energy(item, o, q, c):
        fock_i, dens_i, _, fock_j, dens_j, _ = item
        o_ii, o_ij, o_jj = o
        terms = purified(q[0], c[0]) * o_ii + purified(q[3], c[3]) * o_jj
        terms = terms + (purified(q[1], c[1]) + purified(q[2], c[2]).T) * o_ij
        terms = terms - dens_i.astype(jnp.float32) * fock_i.astype(jnp.float32)
        terms = terms - dens_j.astype(jnp.float32) * fock_j.astype(jnp.float32)
        return jnp.sum(terms)

    o = stage(ortho_blocks, operands)
    s = stage(starts, o)
    q = stage(lambda a: tuple(x.astype(low) for x in times(a, a)), s)
    c = stage(times, q, s)
    return stage(energy, operands, o, q, c)


def lists_kernel(choice_ref, slot_ref, place_ref, load0_ref, list_ref, load_ref):
    mine = place_ref[0]

    @pl.loop(0, load_ref.shape[0])
    def _(d):
        load_ref[d] = load0_ref[d]

    def step(k, filled):
        word = choice_ref[k]
        straight = word & 31
        crossed = lax.shift_right_logical(word, 5) & 31
        free = lax.shift_right_logical(word, 24)
        turn = (load_ref[crossed] < load_ref[straight]) & (free > 0)
        chosen = jnp.where(turn, crossed, straight)
        load_ref[chosen] = load_ref[chosen] + free
        list_ref[0, filled] = lax.shift_right_logical(word, jnp.where(turn, 17, 10)) & 127
        list_ref[1, filled] = slot_ref[k]
        return filled + (chosen == mine).astype(jnp.int32)

    list_ref[2, 0] = lax.fori_loop(0, choice_ref.shape[0], step, 0, unroll=4)


def dimer_lists(group_pairs, group_assign, owner_map, base, x, z, width, depth):
    count = group_pairs.shape[1]
    members = width * depth
    assert (width, depth) == (4, 8)
    fragments = jnp.arange(owner_map.shape[0], dtype=jnp.int32)
    rows = jnp.sum(
        jnp.where(group_pairs[:, :, None] == fragments, owner_map, 0), axis=2, dtype=jnp.int32
    ) - base
    first, second = rows[0], rows[1]
    foreign = (second >= members).astype(jnp.int32)
    second = second - members * foreign
    x_i, z_i = first >> 3, first & 7
    x_j, z_j = second >> 3, second & 7
    straight = x_i * 8 + z_j
    crossed = x_j * 8 + z_i
    near_i, near_j = (z - z_i) & 7, (z - z_j) & 7
    side_i, side_j = (x - x_i) & 3, (x - x_j) & 3
    straight_code = near_i | (8 + 4 * foreign + side_j) << 3
    crossed_code = side_i | near_j << 2
    choice = straight | crossed << 5 | straight_code << 10 | crossed_code << 17 | (1 - foreign) << 24
    order = jnp.arange(count, dtype=jnp.int32)
    same = group_assign[:, None] == group_assign[None, :]
    slot = jnp.sum((same & (order[None, :] < order[:, None])).astype(jnp.int32), axis=1)
    devices = jnp.arange(members, dtype=jnp.int32)
    load = jnp.sum(jnp.where(straight[None, :] == devices[:, None], foreign[None, :], 0), axis=1)
    smem = pl.BlockSpec(memory_space=pltpu.SMEM)
    return pl.pallas_call(
        lists_kernel,
        in_specs=[smem] * 4,
        out_specs=smem,
        out_shape=jax.ShapeDtypeStruct((3, count + LANES), jnp.int32),
        scratch_shapes=[pltpu.SMEM((members,), jnp.int32)],
        cost_estimate=pl.CostEstimate(flops=2 * 10**9, bytes_accessed=count * 32, transcendentals=0),
        name="dimer_lists",
    )(choice, group_assign << 5 | slot, (x * depth + z)[None], load)


def dimers_kernel(layout, list_ref, *refs):
    sources, (out_ref, fock_ref, dens_ref, ortho_ref) = refs[:-4], refs[-4:]
    pools = (fock_ref, dens_ref, ortho_ref)
    members, lanes = out_ref.shape
    for pool, entry, source, index in layout:
        pools[pool][entry] = sources[source][index]
    rows = lax.broadcasted_iota(jnp.int32, (members, lanes), 0)
    columns = lax.broadcasted_iota(jnp.int32, (members, lanes), 1)
    out_ref[...] = jnp.zeros_like(out_ref)
    count = list_ref[2, 0]

    @pl.loop(0, (count + 1) >> 1)
    def _(pair):
        operands, heres = [], []
        for part in range(2):
            position = 2 * pair + part
            real = position < count
            position = jnp.where(real, position, 0)
            word, place = list_ref[0, position], list_ref[1, position]
            straight = word >= 64
            i = jnp.where(straight, word & 7, 8 + (word & 3))
            j = jnp.where(straight, lax.shift_right_logical(word, 3), lax.shift_right_logical(word, 2))
            operands.append(
                (fock_ref[i], dens_ref[i], ortho_ref[i], fock_ref[j], dens_ref[j], ortho_ref[j])
            )
            target, slot = lax.shift_right_logical(place, 5), place & 31
            here = ((rows == target) & (columns == slot)) | (columns == lanes - 1)
            heres.append(here & real)
        energies = dimer_terms(operands)
        update = out_ref[...]
        for here, energy in zip(heres, energies):
            update = update + jnp.where(here, energy, 0.0)
        out_ref[...] = update


def dimer_energies(lists, fock, dens, ortho, members):
    arrays, layout = [], []
    for pool, entries in enumerate((fock, dens, ortho)):
        for entry, (array, index) in enumerate(entries):
            where = next((k for k, a in enumerate(arrays) if a is array), len(arrays))
            if where == len(arrays):
                arrays.append(array)
            layout.append((pool, entry, where, index))
    size = arrays[0].shape[1]
    flops = 14 * 26 * 2 * size**3
    vmem = pl.BlockSpec(memory_space=pltpu.VMEM)
    return pl.pallas_call(
        functools.partial(dimers_kernel, layout),
        in_specs=[pl.BlockSpec(memory_space=pltpu.SMEM)] + [vmem] * len(arrays),
        out_specs=vmem,
        out_shape=jax.ShapeDtypeStruct((members, LANES), jnp.float32),
        scratch_shapes=[pltpu.VMEM((16, size, size), jnp.bfloat16)] * 3,
        compiler_params=pltpu.CompilerParams(vmem_limit_bytes=40 * 1024 * 1024),
        cost_estimate=pl.CostEstimate(flops=flops, bytes_accessed=16 * 6 * size**2, transcendentals=0),
        name="dimer_energies",
    )(lists, *arrays)


def on_device(
    densities,
    core_hamiltonian,
    embedding,
    fit_factors,
    orthogonalizers,
    pairs,
    assignment,
    owner_map,
):
    width, depth = lax.axis_size("dev_0"), lax.axis_size("dev_1")
    members = width * depth
    group_index = lax.axis_index("grp")
    basis_size = densities.shape[1]
    aux_count = fit_factors.shape[0]
    flat_fit = fit_factors.reshape(aux_count, basis_size * basis_size)

    dens_column = along_line(densities, "dev_0")
    pieces = along_ring(jnp.concatenate(dens_column), "dev_1")
    dens_row = [p[:1] for p in pieces]
    gathered = jnp.concatenate(pieces)
    flat_dens = gathered.reshape(members, basis_size * basis_size)
    coeffs = lax.dot_general(
        flat_dens, flat_fit, (((1,), (1,)), ((), ())), preferred_element_type=jnp.float32
    ).astype(jnp.bfloat16)
    coeffs = coeffs.reshape(depth, width, aux_count).swapaxes(0, 1).reshape(members, aux_count)
    terms = jnp.einsum(
        "rp,pmn->rmn", coeffs, fit_factors, preferred_element_type=jnp.float32
    ).astype(jnp.bfloat16)
    chunks = [terms[k * depth : (k + 1) * depth] for k in range(width)]
    column_sum = summed_columns(chunks, "dev_0")
    coulomb = summed_behind([column_sum[k : k + 1] for k in range(depth)], "dev_1")
    fock = (
        core_hamiltonian.astype(jnp.float32) + embedding.astype(jnp.float32) + coulomb
    ).astype(jnp.bfloat16)

    ortho_row = along_line(orthogonalizers, "dev_1")
    ortho_column = along_line(orthogonalizers, "dev_0")
    next_dens = from_behind(jnp.concatenate(dens_column), "grp", -1)
    next_ortho = from_behind(jnp.concatenate(ortho_column), "grp", -1)
    fock_column = along_line(fock, "dev_0")
    fock_row = along_line(fock, "dev_1")
    next_fock = from_behind(jnp.concatenate(fock_column), "grp", -1)

    dim_group = pairs.shape[0] // lax.axis_size("grp")
    start = group_index * dim_group
    group_pairs = lax.dynamic_slice_in_dim(pairs.T, start, dim_group, 1)
    group_assign = lax.dynamic_slice_in_dim(assignment, start, dim_group, 0)
    lists = dimer_lists(
        group_pairs,
        group_assign,
        owner_map,
        (group_index * members).astype(jnp.int32),
        lax.axis_index("dev_0").astype(jnp.int32),
        lax.axis_index("dev_1").astype(jnp.int32),
        width,
        depth,
    )

    def whole(arrays):
        return [(a, 0) for a in arrays]

    def parts(array):
        return [(array, k) for k in range(array.shape[0])]

    sent = dimer_energies(
        lists,
        whole(fock_row + fock_column) + parts(next_fock),
        whole(dens_row + dens_column) + parts(next_dens),
        whole(ortho_row + ortho_column) + parts(next_ortho),
        members,
    )
    arrived = lax.all_to_all(
        sent.reshape(members, 1, LANES), DEV, split_axis=0, concat_axis=0, tiled=True
    )
    mine = jnp.sum(arrived, axis=(0, 1))
    group_sums = sent_to_all(mine[LANES - 1 :], "grp")
    return (mine[:SLOTS], jnp.sum(group_sums))


def solution(mesh):
    torus = Mesh(mesh.devices.reshape(mesh.shape["grp"], 4, 8), ("grp", "dev_0", "dev_1"))
    in_specs = (
        P(GRP_DEV, None, None),
        P(GRP_DEV, None, None),
        P(GRP_DEV, None, None),
        P(DEV, None, None),
        P(GRP_DEV, None, None),
        P(),
        P(),
        P(),
    )
    out_specs = (P(GRP_DEV), P())

    return jax.shard_map(on_device, mesh=torus, in_specs=in_specs, out_specs=out_specs, check_vma=False)
```

```python
import functools

import jax
import jax.numpy as jnp
from jax import lax
from jax.experimental import pallas as pl
from jax.experimental.pallas import tpu as pltpu
from jax.sharding import Mesh
from jax.sharding import PartitionSpec as P

SLOTS = 24
LANES = 128
DEV = ("dev_0", "dev_1")
GRP_DEV = ("grp", "dev_0", "dev_1")
HALF_WIDTH = 4.0


def moved(block, axis, distance):
    count = lax.axis_size(axis)
    return lax.ppermute(block, axis, [(i, (i + distance) % count) for i in range(count)])


def from_behind(block, axis, distance):
    devices = range(lax.axis_size(axis))
    route = [(i - distance, i) for i in devices if i - distance in devices]
    return lax.ppermute(block, axis, route)


def along_ring(block, axis):
    half = lax.axis_size(axis) // 2
    behind, ahead = [block], [block]
    for _ in range(half - 1):
        behind.append(moved(behind[-1], axis, 1))
        ahead.append(moved(ahead[-1], axis, -1))
    cut = block.shape[0] // 2
    far = jnp.concatenate([moved(behind[-1][:cut], axis, 1), moved(ahead[-1][cut:], axis, -1)])
    return behind + [far] + ahead[:0:-1]


def along_line(block, axis):
    return [block] + [moved(block, axis, k) for k in range(1, lax.axis_size(axis))]


def summed_columns(terms, axis):
    cut = terms[0].shape[1] // 16 * 8 + 8
    low, high = [t[:, :cut] for t in terms], [t[:, cut:] for t in terms]
    passing_down = moved(low[2], axis, -1)
    passing_up = moved(high[2], axis, 1)
    high_down = moved(high[1], axis, -1)
    low_up = moved(low[3], axis, 1)
    low_down = moved(added(low[1], passing_down), axis, -1)
    high_up = moved(added(high[3], passing_up), axis, 1)
    return jnp.concatenate(
        [added(low[0], low_up, low_down), added(high[0], high_up, high_down)], axis=1
    )


def added(*arrays):
    return functools.reduce(jnp.add, [a.astype(jnp.float32) for a in arrays]).astype(jnp.bfloat16)


def coefficients(dens, fit_factors):
    return jnp.einsum("rmn,pmn->rp", dens, fit_factors, preferred_element_type=jnp.float32)


def exchanged(array, axis):
    return lax.all_to_all(array, axis, split_axis=0, concat_axis=0, tiled=True)


def sent_to_all(array, axis):
    copies = jnp.broadcast_to(array, (lax.axis_size(axis), *array.shape))
    return lax.all_to_all(copies, axis, split_axis=0, concat_axis=0, tiled=True)


def product(left, right):
    return jnp.dot(left, right, preferred_element_type=jnp.float32)


def turned(left, right):
    return lax.dot_general(
        left, right, (((0,), (0,)), ((), ())), preferred_element_type=jnp.float32
    )


def stage(function, *lists):
    return [function(*items) for items in zip(*lists)]


def dimer_terms(operands):
    size = operands[0][0].shape[0]
    low = jnp.bfloat16
    rows = lax.broadcasted_iota(jnp.int32, (size, size), 0)
    columns = lax.broadcasted_iota(jnp.int32, (size, size), 1)
    middle = jnp.where(rows == columns, 0.5, 0.0).astype(jnp.float32)
    scale = 1.0 / (2.0 * HALF_WIDTH)

    def ortho_blocks(item):
        fock_i, dens_i, ortho_i, fock_j, dens_j, ortho_j = item
        half_ii = product(fock_i, ortho_i).astype(low)
        half_jj = product(fock_j, ortho_j).astype(low)
        coupling = (0.5 * (product(fock_i, dens_j) + product(dens_i, fock_j))).astype(low)
        half_ij = product(coupling, ortho_j).astype(low)
        return turned(ortho_i, half_ii), turned(ortho_i, half_ij), turned(ortho_j, half_jj)

    def starts(blocks):
        o_ii, o_ij, o_jj = blocks
        s_ij = -o_ij * scale
        return (
            (middle - o_ii * scale).astype(low),
            s_ij.astype(low),
            s_ij.T.astype(low),
            (middle - o_jj * scale).astype(low),
        )

    def times(a, b):
        return (
            product(a[0], b[0]) + product(a[1], b[2]),
            product(a[0], b[1]) + product(a[1], b[3]),
            product(a[2], b[0]) + product(a[3], b[2]),
            product(a[2], b[1]) + product(a[3], b[3]),
        )

    def purified(q, c):
        return (3.0 * q.astype(jnp.float32) - 2.0 * c).astype(low).astype(jnp.float32)

    def energy(item, o, q, c):
        fock_i, dens_i, _, fock_j, dens_j, _ = item
        o_ii, o_ij, o_jj = o
        terms = purified(q[0], c[0]) * o_ii + purified(q[3], c[3]) * o_jj
        terms = terms + (purified(q[1], c[1]) + purified(q[2], c[2]).T) * o_ij
        terms = terms - dens_i.astype(jnp.float32) * fock_i.astype(jnp.float32)
        terms = terms - dens_j.astype(jnp.float32) * fock_j.astype(jnp.float32)
        return jnp.sum(terms)

    o = stage(ortho_blocks, operands)
    s = stage(starts, o)
    q = stage(lambda a: tuple(x.astype(low) for x in times(a, a)), s)
    c = stage(times, q, s)
    return stage(energy, operands, o, q, c)


def lists_kernel(choice_ref, slot_ref, place_ref, load0_ref, list_ref, load_ref):
    mine = place_ref[0]
    list_ref[2, 1] = mine & 7

    @pl.loop(0, load_ref.shape[0])
    def _(d):
        load_ref[d] = load0_ref[d]

    def step(k, filled):
        word = choice_ref[k]
        straight = word & 31
        crossed = lax.shift_right_logical(word, 5) & 31
        free = lax.shift_right_logical(word, 24)
        turn = (load_ref[crossed] < load_ref[straight]) & (free > 0)
        chosen = jnp.where(turn, crossed, straight)
        load_ref[chosen] = load_ref[chosen] + free
        list_ref[0, filled] = lax.shift_right_logical(word, jnp.where(turn, 17, 10)) & 127
        list_ref[1, filled] = slot_ref[k]
        return filled + (chosen == mine).astype(jnp.int32)

    list_ref[2, 0] = lax.fori_loop(0, choice_ref.shape[0], step, 0, unroll=4)


def dimer_lists(group_pairs, group_assign, owner_map, base, x, z, width, depth):
    count = group_pairs.shape[1]
    members = width * depth
    assert (width, depth) == (4, 8)
    fragments = jnp.arange(owner_map.shape[0], dtype=jnp.int32)
    rows = jnp.sum(
        jnp.where(group_pairs[:, :, None] == fragments, owner_map, 0), axis=2, dtype=jnp.int32
    ) - base
    first, second = rows[0], rows[1]
    foreign = (second >= members).astype(jnp.int32)
    second = second - members * foreign
    x_i, z_i = first >> 3, first & 7
    x_j, z_j = second >> 3, second & 7
    straight = x_i * 8 + z_j
    crossed = x_j * 8 + z_i
    near_i, near_j = (z - z_i) & 7, (z - z_j) & 7
    side_i, side_j = (x - x_i) & 3, (x - x_j) & 3
    straight_code = near_i | (8 + 4 * foreign + side_j) << 3
    crossed_code = side_i | near_j << 2
    choice = straight | crossed << 5 | straight_code << 10 | crossed_code << 17 | (1 - foreign) << 24
    order = jnp.arange(count, dtype=jnp.int32)
    same = group_assign[:, None] == group_assign[None, :]
    slot = jnp.sum((same & (order[None, :] < order[:, None])).astype(jnp.int32), axis=1)
    devices = jnp.arange(members, dtype=jnp.int32)
    load = jnp.sum(jnp.where(straight[None, :] == devices[:, None], foreign[None, :], 0), axis=1)
    smem = pl.BlockSpec(memory_space=pltpu.SMEM)
    return pl.pallas_call(
        lists_kernel,
        in_specs=[smem] * 4,
        out_specs=smem,
        out_shape=jax.ShapeDtypeStruct((3, count + LANES), jnp.int32),
        scratch_shapes=[pltpu.SMEM((members,), jnp.int32)],
        cost_estimate=pl.CostEstimate(flops=2 * 10**9, bytes_accessed=count * 32, transcendentals=0),
        name="dimer_lists",
    )(choice, group_assign << 5 | slot, (x * depth + z)[None], load)


def dimers_kernel(layout, list_ref, *refs):
    sources, (out_ref, fock_ref, dens_ref, ortho_ref, sems) = refs[:-5], refs[-5:]
    pools = (fock_ref, dens_ref, ortho_ref)
    members, lanes = out_ref.shape
    copies = [
        pltpu.make_async_copy(sources[source].at[index], pools[pool].at[entry], sems.at[pool, entry])
        for pool, entry, source, index in layout
    ]
    for copy in copies:
        copy.start()
    rows = lax.broadcasted_iota(jnp.int32, (members, lanes), 0)
    columns = lax.broadcasted_iota(jnp.int32, (members, lanes), 1)
    out_ref[...] = jnp.zeros_like(out_ref)
    for copy in copies:
        copy.wait()
    count = list_ref[2, 0]
    z = list_ref[2, 1]

    def at(entry):
        return jnp.where(entry < 8, (z - entry) & 7, entry)

    @pl.loop(0, (count + 1) >> 1)
    def _(pair):
        operands, heres = [], []
        for part in range(2):
            position = 2 * pair + part
            real = position < count
            position = jnp.where(real, position, 0)
            word, place = list_ref[0, position], list_ref[1, position]
            straight = word >= 64
            i = jnp.where(straight, word & 7, 8 + (word & 3))
            j = jnp.where(straight, lax.shift_right_logical(word, 3), lax.shift_right_logical(word, 2))
            operands.append(
                (fock_ref[at(i)], dens_ref[i], ortho_ref[at(i)], fock_ref[at(j)], dens_ref[j], ortho_ref[at(j)])
            )
            target, slot = lax.shift_right_logical(place, 5), place & 31
            here = ((rows == target) & (columns == slot)) | (columns == lanes - 1)
            heres.append(here & real)
        energies = dimer_terms(operands)
        update = out_ref[...]
        for here, energy in zip(heres, energies):
            update = update + jnp.where(here, energy, 0.0)
        out_ref[...] = update


def dimer_energies(lists, fock, dens, ortho, members):
    arrays, layout = [], []
    for pool, entries in enumerate((fock, dens, ortho)):
        for entry, (array, index) in enumerate(entries):
            where = next((k for k, a in enumerate(arrays) if a is array), len(arrays))
            if where == len(arrays):
                arrays.append(array)
            layout.append((pool, entry, where, index))
    size = arrays[0].shape[1]
    flops = 14 * 26 * 2 * size**3
    vmem = pl.BlockSpec(memory_space=pltpu.VMEM)
    return pl.pallas_call(
        functools.partial(dimers_kernel, layout),
        in_specs=[pl.BlockSpec(memory_space=pltpu.SMEM)]
        + [pl.BlockSpec(memory_space=pltpu.HBM)] * len(arrays),
        out_specs=vmem,
        out_shape=jax.ShapeDtypeStruct((members, LANES), jnp.float32),
        scratch_shapes=[pltpu.VMEM((16, size, size), jnp.bfloat16)] * 3
        + [pltpu.SemaphoreType.DMA((3, 16))],
        compiler_params=pltpu.CompilerParams(vmem_limit_bytes=62 * 1024 * 1024),
        cost_estimate=pl.CostEstimate(flops=flops, bytes_accessed=16 * 6 * size**2, transcendentals=0),
        name="dimer_energies",
    )(lists, *arrays)


def on_device(
    densities,
    core_hamiltonian,
    embedding,
    fit_factors,
    orthogonalizers,
    pairs,
    assignment,
    owner_map,
):
    width, depth = lax.axis_size("dev_0"), lax.axis_size("dev_1")
    members = width * depth
    group_index = lax.axis_index("grp")

    dens_column = along_line(densities, "dev_0")
    pieces = along_ring(jnp.concatenate(dens_column), "dev_1")
    half = depth // 2
    early = jnp.concatenate(pieces[half + 1 :] + pieces[:half])
    coeffs = [coefficients(rows, fit_factors) for rows in (pieces[half], early)]
    coeffs = jnp.concatenate(coeffs).reshape(depth, width, -1)
    row_index = lax.axis_index("dev_1")
    coeffs = jnp.concatenate([coeffs[::-1], coeffs[::-1]])
    first = (half - 1 - row_index + depth) % depth
    coeffs = lax.dynamic_slice_in_dim(coeffs, first, depth, 0)
    coeffs = coeffs.swapaxes(0, 1).reshape(members, -1).astype(jnp.bfloat16)
    terms = jnp.einsum(
        "rp,pmn->rmn", coeffs, fit_factors, preferred_element_type=jnp.float32
    ).astype(jnp.bfloat16)
    chunks = [terms[k * depth : (k + 1) * depth] for k in range(width)]
    column_sum = summed_columns(chunks, "dev_0")
    coulomb = exchanged(column_sum, "dev_1").astype(jnp.float32).sum(axis=0, keepdims=True)
    fock = (
        core_hamiltonian.astype(jnp.float32) + embedding.astype(jnp.float32) + coulomb
    ).astype(jnp.bfloat16)

    ortho_row = exchanged(jnp.concatenate([orthogonalizers] * depth), "dev_1")
    ortho_column = along_line(orthogonalizers, "dev_0")
    next_dens = from_behind(jnp.concatenate(dens_column), "grp", -1)
    next_ortho = from_behind(jnp.concatenate(ortho_column), "grp", -1)
    fock_column = along_line(fock, "dev_0")
    fock_row = exchanged(jnp.concatenate([fock] * depth), "dev_1")
    next_fock = from_behind(jnp.concatenate(fock_column), "grp", -1)

    dim_group = pairs.shape[0] // lax.axis_size("grp")
    start = group_index * dim_group
    group_pairs = lax.dynamic_slice_in_dim(pairs.T, start, dim_group, 1)
    group_assign = lax.dynamic_slice_in_dim(assignment, start, dim_group, 0)
    lists = dimer_lists(
        group_pairs,
        group_assign,
        owner_map,
        (group_index * members).astype(jnp.int32),
        lax.axis_index("dev_0").astype(jnp.int32),
        lax.axis_index("dev_1").astype(jnp.int32),
        width,
        depth,
    )

    def whole(arrays):
        return [(a, 0) for a in arrays]

    def parts(array):
        return [(array, k) for k in range(array.shape[0])]

    sent = dimer_energies(
        lists,
        parts(fock_row) + whole(fock_column) + parts(next_fock),
        whole(pieces + dens_column) + parts(next_dens),
        parts(ortho_row) + whole(ortho_column) + parts(next_ortho),
        members,
    )
    arrived = lax.all_to_all(
        sent.reshape(members, 1, LANES), DEV, split_axis=0, concat_axis=0, tiled=True
    )
    mine = jnp.sum(arrived, axis=(0, 1))
    group_sums = sent_to_all(mine[LANES - 1 :], "grp")
    return (mine[:SLOTS], jnp.sum(group_sums))


def solution(mesh):
    torus = Mesh(mesh.devices.reshape(mesh.shape["grp"], 4, 8), ("grp", "dev_0", "dev_1"))
    in_specs = (
        P(GRP_DEV, None, None),
        P(GRP_DEV, None, None),
        P(GRP_DEV, None, None),
        P(DEV, None, None),
        P(GRP_DEV, None, None),
        P(),
        P(),
        P(),
    )
    out_specs = (P(GRP_DEV), P())

    return jax.shard_map(on_device, mesh=torus, in_specs=in_specs, out_specs=out_specs, check_vma=False)
```

```python
import functools

import jax
import jax.numpy as jnp
from jax import lax
from jax.experimental import pallas as pl
from jax.experimental.pallas import tpu as pltpu
from jax.sharding import Mesh
from jax.sharding import PartitionSpec as P

SLOTS = 24
LANES = 128
DEV = ("dev_0", "dev_1")
GRP_DEV = ("grp", "dev_0", "dev_1")
HALF_WIDTH = 4.0


def moved(block, axis, distance):
    count = lax.axis_size(axis)
    return lax.ppermute(block, axis, [(i, (i + distance) % count) for i in range(count)])


def from_behind(block, axis, distance):
    devices = range(lax.axis_size(axis))
    route = [(i - distance, i) for i in devices if i - distance in devices]
    return lax.ppermute(block, axis, route)


def along_ring(block, axis):
    half = lax.axis_size(axis) // 2
    behind, ahead = [block], [block]
    for _ in range(half - 1):
        behind.append(moved(behind[-1], axis, 1))
        ahead.append(moved(ahead[-1], axis, -1))
    cut = block.shape[0] // 2
    far = jnp.concatenate([moved(behind[-1][:cut], axis, 1), moved(ahead[-1][cut:], axis, -1)])
    return behind + [far] + ahead[:0:-1]


def along_line(block, axis):
    return [block] + [moved(block, axis, k) for k in range(1, lax.axis_size(axis))]


def summed_columns(terms, axis):
    cut = terms[0].shape[1] // 16 * 8 + 8
    low, high = [t[:, :cut] for t in terms], [t[:, cut:] for t in terms]
    passing_down = moved(low[2], axis, -1)
    passing_up = moved(high[2], axis, 1)
    high_down = moved(high[1], axis, -1)
    low_up = moved(low[3], axis, 1)
    low_down = moved(added(low[1], passing_down), axis, -1)
    high_up = moved(added(high[3], passing_up), axis, 1)
    return jnp.concatenate(
        [added(low[0], low_up, low_down), added(high[0], high_up, high_down)], axis=1
    )


def added(*arrays):
    return functools.reduce(jnp.add, [a.astype(jnp.float32) for a in arrays]).astype(jnp.bfloat16)


def coefficients(dens, fit_factors):
    return jnp.einsum("rmn,pmn->rp", dens, fit_factors, preferred_element_type=jnp.float32)


def exchanged(array, axis):
    return lax.all_to_all(array, axis, split_axis=0, concat_axis=0, tiled=True)


def sent_to_all(array, axis):
    copies = jnp.broadcast_to(array, (lax.axis_size(axis), *array.shape))
    return lax.all_to_all(copies, axis, split_axis=0, concat_axis=0, tiled=True)


def product(left, right):
    return jnp.dot(left, right, preferred_element_type=jnp.float32)


def turned(left, right):
    return lax.dot_general(
        left, right, (((0,), (0,)), ((), ())), preferred_element_type=jnp.float32
    )


def stage(function, *lists):
    return [function(*items) for items in zip(*lists)]


def dimer_terms(operands):
    size = operands[0][0].shape[0]
    low = jnp.bfloat16
    rows = lax.broadcasted_iota(jnp.int32, (size, size), 0)
    columns = lax.broadcasted_iota(jnp.int32, (size, size), 1)
    middle = jnp.where(rows == columns, 0.5, 0.0).astype(jnp.float32)
    scale = 1.0 / (2.0 * HALF_WIDTH)

    def ortho_blocks(item):
        fock_i, dens_i, ortho_i, fock_j, dens_j, ortho_j = item
        half_ii = product(fock_i, ortho_i).astype(low)
        half_jj = product(fock_j, ortho_j).astype(low)
        coupling = (0.5 * (product(fock_i, dens_j) + product(dens_i, fock_j))).astype(low)
        half_ij = product(coupling, ortho_j).astype(low)
        return turned(ortho_i, half_ii), turned(ortho_i, half_ij), turned(ortho_j, half_jj)

    def starts(blocks):
        o_ii, o_ij, o_jj = blocks
        s_ij = -o_ij * scale
        return (
            (middle - o_ii * scale).astype(low),
            s_ij.astype(low),
            s_ij.T.astype(low),
            (middle - o_jj * scale).astype(low),
        )

    def times(a, b):
        return (
            product(a[0], b[0]) + product(a[1], b[2]),
            product(a[0], b[1]) + product(a[1], b[3]),
            product(a[2], b[0]) + product(a[3], b[2]),
            product(a[2], b[1]) + product(a[3], b[3]),
        )

    def purified(q, c):
        return (3.0 * q.astype(jnp.float32) - 2.0 * c).astype(low).astype(jnp.float32)

    def energy(item, o, q, c):
        fock_i, dens_i, _, fock_j, dens_j, _ = item
        o_ii, o_ij, o_jj = o
        terms = purified(q[0], c[0]) * o_ii + purified(q[3], c[3]) * o_jj
        terms = terms + (purified(q[1], c[1]) + purified(q[2], c[2]).T) * o_ij
        terms = terms - dens_i.astype(jnp.float32) * fock_i.astype(jnp.float32)
        terms = terms - dens_j.astype(jnp.float32) * fock_j.astype(jnp.float32)
        return jnp.sum(terms)

    o = stage(ortho_blocks, operands)
    s = stage(starts, o)
    q = stage(lambda a: tuple(x.astype(low) for x in times(a, a)), s)
    c = stage(times, q, s)
    return stage(energy, operands, o, q, c)


def lists_kernel(choice_ref, slot_ref, place_ref, load0_ref, list_ref, load_ref):
    mine = place_ref[0]
    list_ref[2, 1] = mine & 7

    @pl.loop(0, load_ref.shape[0])
    def _(d):
        load_ref[d] = load0_ref[d]

    def step(k, filled):
        word = choice_ref[k]
        straight = word & 31
        crossed = lax.shift_right_logical(word, 5) & 31
        free = lax.shift_right_logical(word, 24)
        turn = (load_ref[crossed] < load_ref[straight]) & (free > 0)
        chosen = jnp.where(turn, crossed, straight)
        load_ref[chosen] = load_ref[chosen] + free
        list_ref[0, filled] = lax.shift_right_logical(word, jnp.where(turn, 17, 10)) & 127
        list_ref[1, filled] = slot_ref[k]
        return filled + (chosen == mine).astype(jnp.int32)

    list_ref[2, 0] = lax.fori_loop(0, choice_ref.shape[0], step, 0, unroll=4)


def dimer_lists(group_pairs, group_assign, owner_map, base, x, z, width, depth):
    count = group_pairs.shape[1]
    members = width * depth
    assert (width, depth) == (4, 8)
    fragments = jnp.arange(owner_map.shape[0], dtype=jnp.int32)
    rows = jnp.sum(
        jnp.where(group_pairs[:, :, None] == fragments, owner_map, 0), axis=2, dtype=jnp.int32
    ) - base
    first, second = rows[0], rows[1]
    foreign = (second >= members).astype(jnp.int32)
    second = second - members * foreign
    x_i, z_i = first >> 3, first & 7
    x_j, z_j = second >> 3, second & 7
    straight = x_i * 8 + z_j
    crossed = x_j * 8 + z_i
    near_i, near_j = (z - z_i) & 7, (z - z_j) & 7
    side_i, side_j = (x - x_i) & 3, (x - x_j) & 3
    straight_code = near_i | (8 + 4 * foreign + side_j) << 3
    crossed_code = side_i | near_j << 2
    choice = straight | crossed << 5 | straight_code << 10 | crossed_code << 17 | (1 - foreign) << 24
    order = jnp.arange(count, dtype=jnp.int32)
    same = group_assign[:, None] == group_assign[None, :]
    slot = jnp.sum((same & (order[None, :] < order[:, None])).astype(jnp.int32), axis=1)
    devices = jnp.arange(members, dtype=jnp.int32)
    load = jnp.sum(jnp.where(straight[None, :] == devices[:, None], foreign[None, :], 0), axis=1)
    smem = pl.BlockSpec(memory_space=pltpu.SMEM)
    return pl.pallas_call(
        lists_kernel,
        in_specs=[smem] * 4,
        out_specs=smem,
        out_shape=jax.ShapeDtypeStruct((3, count + LANES), jnp.int32),
        scratch_shapes=[pltpu.SMEM((members,), jnp.int32)],
        cost_estimate=pl.CostEstimate(flops=2 * 10**9, bytes_accessed=count * 32, transcendentals=0),
        name="dimer_lists",
    )(choice, group_assign << 5 | slot, (x * depth + z)[None], load)


def dimers_kernel(layout, list_ref, *refs):
    sources, (out_ref, fock_ref, dens_ref, ortho_ref, sems) = refs[:-5], refs[-5:]
    pools = (fock_ref, dens_ref, ortho_ref)
    members, lanes = out_ref.shape
    copies = [
        pltpu.make_async_copy(sources[source].at[index], pools[pool].at[entry], sems.at[pool, entry])
        for pool, entry, source, index in layout
    ]
    for copy in copies:
        copy.start()
    rows = lax.broadcasted_iota(jnp.int32, (members, lanes), 0)
    columns = lax.broadcasted_iota(jnp.int32, (members, lanes), 1)
    out_ref[...] = jnp.zeros_like(out_ref)
    for copy in copies:
        copy.wait()
    count = list_ref[2, 0]
    z = list_ref[2, 1]

    def at(entry):
        return jnp.where(entry < 8, (z - entry) & 7, entry)

    @pl.loop(0, (count + 1) >> 1)
    def _(pair):
        operands, heres = [], []
        for part in range(2):
            position = 2 * pair + part
            real = position < count
            position = jnp.where(real, position, 0)
            word, place = list_ref[0, position], list_ref[1, position]
            straight = word >= 64
            i = jnp.where(straight, word & 7, 8 + (word & 3))
            j = jnp.where(straight, lax.shift_right_logical(word, 3), lax.shift_right_logical(word, 2))
            operands.append(
                (fock_ref[at(i)], dens_ref[i], ortho_ref[i], fock_ref[at(j)], dens_ref[j], ortho_ref[j])
            )
            target, slot = lax.shift_right_logical(place, 5), place & 31
            here = ((rows == target) & (columns == slot)) | (columns == lanes - 1)
            heres.append(here & real)
        energies = dimer_terms(operands)
        update = out_ref[...]
        for here, energy in zip(heres, energies):
            update = update + jnp.where(here, energy, 0.0)
        out_ref[...] = update


def dimer_energies(lists, fock, dens, ortho, members):
    arrays, layout = [], []
    for pool, entries in enumerate((fock, dens, ortho)):
        for entry, (array, index) in enumerate(entries):
            where = next((k for k, a in enumerate(arrays) if a is array), len(arrays))
            if where == len(arrays):
                arrays.append(array)
            layout.append((pool, entry, where, index))
    size = arrays[0].shape[1]
    flops = 14 * 26 * 2 * size**3
    vmem = pl.BlockSpec(memory_space=pltpu.VMEM)
    return pl.pallas_call(
        functools.partial(dimers_kernel, layout),
        in_specs=[pl.BlockSpec(memory_space=pltpu.SMEM)]
        + [pl.BlockSpec(memory_space=pltpu.HBM)] * len(arrays),
        out_specs=vmem,
        out_shape=jax.ShapeDtypeStruct((members, LANES), jnp.float32),
        scratch_shapes=[pltpu.VMEM((16, size, size), jnp.bfloat16)] * 3
        + [pltpu.SemaphoreType.DMA((3, 16))],
        compiler_params=pltpu.CompilerParams(vmem_limit_bytes=62 * 1024 * 1024),
        cost_estimate=pl.CostEstimate(flops=flops, bytes_accessed=16 * 6 * size**2, transcendentals=0),
        name="dimer_energies",
    )(lists, *arrays)


def on_device(
    densities,
    core_hamiltonian,
    embedding,
    fit_factors,
    orthogonalizers,
    pairs,
    assignment,
    owner_map,
):
    width, depth = lax.axis_size("dev_0"), lax.axis_size("dev_1")
    members = width * depth
    group_index = lax.axis_index("grp")

    dens_column = along_line(densities, "dev_0")
    pieces = along_ring(jnp.concatenate(dens_column), "dev_1")
    half = depth // 2
    early = jnp.concatenate(pieces[half + 1 :] + pieces[:half])
    coeffs = [coefficients(rows, fit_factors) for rows in (pieces[half], early)]
    coeffs = jnp.concatenate(coeffs).reshape(depth, width, -1)
    row_index = lax.axis_index("dev_1")
    coeffs = jnp.concatenate([coeffs[::-1], coeffs[::-1]])
    first = (half - 1 - row_index + depth) % depth
    coeffs = lax.dynamic_slice_in_dim(coeffs, first, depth, 0)
    coeffs = coeffs.swapaxes(0, 1).reshape(members, -1).astype(jnp.bfloat16)
    terms = jnp.einsum(
        "rp,pmn->rmn", coeffs, fit_factors, preferred_element_type=jnp.float32
    ).astype(jnp.bfloat16)
    chunks = [terms[k * depth : (k + 1) * depth] for k in range(width)]
    column_sum = summed_columns(chunks, "dev_0")
    coulomb = exchanged(column_sum, "dev_1").astype(jnp.float32).sum(axis=0, keepdims=True)
    fock = (
        core_hamiltonian.astype(jnp.float32) + embedding.astype(jnp.float32) + coulomb
    ).astype(jnp.bfloat16)

    ortho_row = along_line(orthogonalizers, "dev_1")
    ortho_column = along_line(orthogonalizers, "dev_0")
    next_dens = from_behind(jnp.concatenate(dens_column), "grp", -1)
    next_ortho = from_behind(jnp.concatenate(ortho_column), "grp", -1)
    fock_column = along_line(fock, "dev_0")
    fock_row = exchanged(jnp.concatenate([fock] * depth), "dev_1")
    next_fock = from_behind(jnp.concatenate(fock_column), "grp", -1)

    dim_group = pairs.shape[0] // lax.axis_size("grp")
    start = group_index * dim_group
    group_pairs = lax.dynamic_slice_in_dim(pairs.T, start, dim_group, 1)
    group_assign = lax.dynamic_slice_in_dim(assignment, start, dim_group, 0)
    lists = dimer_lists(
        group_pairs,
        group_assign,
        owner_map,
        (group_index * members).astype(jnp.int32),
        lax.axis_index("dev_0").astype(jnp.int32),
        lax.axis_index("dev_1").astype(jnp.int32),
        width,
        depth,
    )

    def whole(arrays):
        return [(a, 0) for a in arrays]

    def parts(array):
        return [(array, k) for k in range(array.shape[0])]

    sent = dimer_energies(
        lists,
        parts(fock_row) + whole(fock_column) + parts(next_fock),
        whole(pieces + dens_column) + parts(next_dens),
        whole(ortho_row + ortho_column) + parts(next_ortho),
        members,
    )
    arrived = lax.all_to_all(
        sent.reshape(members, 1, LANES), DEV, split_axis=0, concat_axis=0, tiled=True
    )
    mine = jnp.sum(arrived, axis=(0, 1))
    group_sums = sent_to_all(mine[LANES - 1 :], "grp")
    return (mine[:SLOTS], jnp.sum(group_sums))


def solution(mesh):
    torus = Mesh(mesh.devices.reshape(mesh.shape["grp"], 4, 8), ("grp", "dev_0", "dev_1"))
    in_specs = (
        P(GRP_DEV, None, None),
        P(GRP_DEV, None, None),
        P(GRP_DEV, None, None),
        P(DEV, None, None),
        P(GRP_DEV, None, None),
        P(),
        P(),
        P(),
    )
    out_specs = (P(GRP_DEV), P())

    return jax.shard_map(on_device, mesh=torus, in_specs=in_specs, out_specs=out_specs, check_vma=False)
```
